32 devices in a mesh: row: 4 (over z), col: 4 (over x, core), depth: 2 (over y).
Axes of the slice: x: 2, y: 2, z: 4, core: 2. Of those that a mesh axis runs over, the one named last changes fastest.
Arguments:
- diag_block: float32 [512, 512], P(('row', 'col')), may hold values from -40 to 60, as said below
- panel: float32 [16384, 512], P(('row', 'col'), 'depth'), may hold values from -1.2 to 1.2
- trailing: float32 [16384, 16384], P(('col', 'depth'), 'row'), may hold values from -6 to 6
Outputs:
- factor_diag: float32 [512, 512], P(('row', 'col'))
- factor_panel: float32 [16384, 512], P(('row', 'col'), 'depth')
- schur: float32 [16384, 16384], P(('col', 'depth'), 'row')
The draws below stay inside these ranges and needn't reach their ends.
Inputs may be any that keep to these rules, and one draw needn't show every extreme that they name: `diag_block`: symmetric, with every eigenvalue 1 or more.
All inputs are finite; a program needn't handle non-finite values.
Results may differ from the reference program's by a relative error of at most 0.000071.
Values sent between devices are 32-bit elements; how exact they have to be, the bound alone decides.
A program may use at most 128 MiB of HBM per device.

```python
import jax
import jax.numpy as jnp
from jax import lax

TRAIL = 16384
BLOCK = 512


def draw_diag_block(key, part):
    base = jax.random.normal(jax.random.fold_in(key, 11), (BLOCK, BLOCK), jnp.float32)
    gram = jnp.dot(base, base.T, precision=lax.Precision.HIGHEST) / BLOCK
    result = 0.5 * (gram + gram.T) + jnp.eye(BLOCK, dtype=jnp.float32)
    return result


def levels(stream_key, shape, cuts, smallest, top_value):
    gain = 1.0
    for dim, parts in cuts:
        heights = jax.random.uniform(jax.random.fold_in(jax.random.fold_in(stream_key, 6), dim), (parts,), jnp.float32, smallest / len(cuts), top_value / len(cuts))
        gain = gain * jnp.repeat(jnp.exp(heights), shape[dim] // parts).reshape((-1,) + (1,) * (len(shape) - 1 - dim))
    return gain


def centred(key, extent, width, limit, cuts=(), kind=jnp.bfloat16):
    values = width * jax.random.normal(key, extent, jnp.float32)
    if cuts:
        values = values * levels(key, extent, cuts, -0.22, 0.18)
    return jnp.clip(values, -limit, limit).astype(kind)


def setup_inputs(seed: int = 0) -> dict:
    keys = jax.random.split(jax.random.key(seed), 4)
    return {
        "diag_block": draw_diag_block(jax.random.fold_in(keys[3], 71), 0),
        "panel": centred(keys[1], (TRAIL, BLOCK), 0.2, 1.2, ((0, 16), (1, 2)), jnp.float32),
        "trailing": centred(keys[2], (TRAIL, TRAIL), 1.0, 6.0, ((0, 8), (1, 4)), jnp.float32),
    }


def outer_rows(left, right):
    return lax.dot_general(left.astype(jnp.float32), right.astype(jnp.float32), (((1,), (1,)), ((), ())), precision=lax.Precision.HIGHEST, preferred_element_type=jnp.float32)

def reference(diag_block, panel, trailing):
    lower = jnp.linalg.cholesky(diag_block)
    ident = jnp.eye(BLOCK, dtype=jnp.float32)
    inverse = lax.linalg.triangular_solve(lower, ident, left_side=True, lower=True)
    factor_panel = jnp.dot(panel.astype(jnp.float32), inverse.T.astype(jnp.float32), precision=lax.Precision.HIGHEST, preferred_element_type=jnp.float32)
    step = min(TRAIL, 1024)
    count = TRAIL // step
    trail_blocks = trailing.reshape(count, step, TRAIL)
    panel_blocks = factor_panel.reshape(count, step, BLOCK)

    def update(pair):
        return pair[0] - outer_rows(pair[1], factor_panel)
    schur = lax.map(update, (trail_blocks, panel_blocks)).reshape(TRAIL, TRAIL)
    return (lower, factor_panel, schur)
```

```python
import jax
import jax.numpy as jnp
from jax import lax
from jax.experimental import pallas as pl
from jax.experimental.pallas import tpu as pltpu
from jax.sharding import PartitionSpec as P


BLOCK = 128
GROUP = 8


def dot_t(left, right, precision):
    return lax.dot_general(
        left,
        right,
        (((1,), (1,)), ((), ())),
        precision=precision,
        preferred_element_type=jnp.float32,
    )


def factor_block(work, inv):
    size = work.shape[0]
    sub = lax.broadcasted_iota(jnp.int32, (GROUP, size), 0)
    tall = lax.broadcasted_iota(jnp.int32, (size, GROUP), 0)
    diag_rows = lax.broadcasted_iota(jnp.int32, (size, size), 0)
    diag_cols = lax.broadcasted_iota(jnp.int32, (size, size), 1)
    inv[...] = jnp.where(diag_rows == diag_cols, 1.0, 0.0)

    @pl.loop(0, size // GROUP)
    def _(g):
        base = pl.multiple_of(g * GROUP, GROUP)
        rows = work[pl.ds(base, GROUP), :]
        inv_rows = inv[pl.ds(base, GROUP), :]
        pivot = pltpu.roll(rows, lax.rem(size - base, size), 1)
        cols = [jnp.broadcast_to(pivot[:, k : k + 1], (GROUP, size)) for k in range(GROUP)]
        for k in range(GROUP):
            scale = lax.rsqrt(cols[k][k : k + 1, :])
            low = cols[k] * scale
            row = rows[k : k + 1, :] * scale
            inv_row = inv_rows[k : k + 1, :] * scale
            rows = jnp.where(sub > k, rows - low * row, jnp.where(sub == k, row, rows))
            inv_rows = jnp.where(
                sub > k, inv_rows - low * inv_row, jnp.where(sub == k, inv_row, inv_rows)
            )
            for m in range(k + 1, GROUP):
                cols[m] = cols[m] - low * low[m : m + 1, :]
        below = jnp.where(tall >= base + GROUP, rows.T, 0.0)
        new_work = work[...]
        new_inv = inv[...]
        for k in range(GROUP):
            wide = jnp.broadcast_to(below[:, k : k + 1], (size, size))
            new_work = new_work - wide * rows[k : k + 1, :]
            new_inv = new_inv - wide * inv_rows[k : k + 1, :]
        work[...] = new_work
        inv[...] = new_inv
        work[pl.ds(base, GROUP), :] = rows
        inv[pl.ds(base, GROUP), :] = inv_rows


def cholesky_kernel(a_ref, lower_ref, inverse_ref, rest, work, inv):
    n = a_ref.shape[0]
    high = lax.Precision.HIGHEST
    rest[...] = a_ref[...]
    lower_ref[...] = jnp.zeros_like(lower_ref)
    inverse_ref[...] = jnp.zeros_like(inverse_ref)
    rows = lax.broadcasted_iota(jnp.int32, (BLOCK, BLOCK), 0)
    cols = lax.broadcasted_iota(jnp.int32, (BLOCK, BLOCK), 1)
    for start in range(0, n, BLOCK):
        stop = start + BLOCK
        work[...] = rest[start:stop, start:stop]
        factor_block(work, inv)
        lower_ref[start:stop, start:stop] = jnp.where(cols >= rows, work[...], 0.0).T
        inverse_ref[start:stop, start:stop] = inv[...]
        if stop < n:
            panel = dot_t(rest[stop:, start:stop], inv[...], high)
            lower_ref[stop:, start:stop] = panel
            rest[stop:, stop:] = rest[stop:, stop:] - dot_t(panel, panel, high)
        if start:
            known = jnp.dot(
                lower_ref[start:stop, :start],
                inverse_ref[:start, :start],
                precision=high,
                preferred_element_type=jnp.float32,
            )
            inverse_ref[start:stop, :start] = -jnp.dot(
                inv[...], known, precision=high, preferred_element_type=jnp.float32
            )


def cholesky_and_inverse(a):
    n = a.shape[0]
    whole = jax.ShapeDtypeStruct((n, n), jnp.float32)
    return pl.pallas_call(
        cholesky_kernel,
        out_shape=(whole, whole),
        in_specs=[pl.BlockSpec(memory_space=pltpu.VMEM)],
        out_specs=(pl.BlockSpec(memory_space=pltpu.VMEM),) * 2,
        scratch_shapes=[
            pltpu.VMEM((n, n), jnp.float32),
            pltpu.VMEM((BLOCK, BLOCK), jnp.float32),
            pltpu.VMEM((BLOCK, BLOCK), jnp.float32),
        ],
        compiler_params=pltpu.CompilerParams(vmem_limit_bytes=16 * 1024 * 1024),
        cost_estimate=pl.CostEstimate(
            flops=100_000_000_000, bytes_accessed=3 * 4 * n * n, transcendentals=0
        ),
        name="cholesky_and_inverse",
    )(a)


def solve(pieces, inverse):
    width = pieces.shape[2]
    total = None
    for h in range(pieces.shape[0]):
        part = dot_t(pieces[h], inverse[:, h * width : (h + 1) * width], lax.Precision.HIGH)
        total = part if total is None else total + part
    return total


def gather_diag(mine):
    n_row, n_col = lax.axis_size("row"), lax.axis_size("col")
    rows, width = mine.shape[0] // n_row, mine.shape[1]
    half = width // 2
    halves = [
        lax.all_gather(mine[:, k : k + half], "col", axis=0, tiled=False)
        for k in range(0, width, half)
    ]
    whole = jnp.concatenate(halves, axis=2).reshape(n_col, n_row, rows, width)
    return whole.transpose(1, 0, 2, 3).reshape(n_row * n_col * rows, width)


def local(diag_block, panel, trailing):
    n_row, n_col, n_depth = (lax.axis_size(name) for name in ("row", "col", "depth"))
    per_target = n_row // n_depth
    pairs = []
    for r in range(n_row):
        for c in range(n_col):
            for d in range(n_depth):
                block = r * n_col + c
                target = block // per_target
                to_row = block % per_target * n_depth + d
                to = (to_row * n_col + target // n_depth) * n_depth + target % n_depth
                pairs.append(((r * n_col + c) * n_depth + d, to))

    height, width = panel.shape
    diag_rows = lax.all_gather(diag_block, "row", axis=0, tiled=True)
    whole_diag = gather_diag(diag_rows)
    moved = lax.ppermute(panel, ("row", "col", "depth"), pairs)
    whole_diag, moved, late = lax.optimization_barrier((whole_diag, moved, panel))
    across = lax.all_gather(late, ("depth", "col"), axis=0, tiled=False)
    across = across.reshape(n_depth, n_col * height, width)

    me = lax.axis_index("row")
    up = [(r, (r + 1) % n_row) for r in range(n_row)]
    down = [(r, (r + n_row - 1) % n_row) for r in range(n_row)]

    def place(whole, piece, source, offset):
        at = (source % n_depth, source // n_depth * height + offset, 0)
        return lax.dynamic_update_slice(whole, piece[None], at)

    along = jnp.zeros((n_depth, per_target * height, width), jnp.float32)
    along = place(along, moved, me, 0)
    from_below = from_above = moved
    for step in range(1, (n_row - 1) // 2 + 1):
        from_below = lax.ppermute(from_below, "row", up)
        from_above = lax.ppermute(from_above, "row", down)
        along = place(along, from_below, (me + n_row - step) % n_row, 0)
        along = place(along, from_above, (me + step) % n_row, 0)
    if n_row % 2 == 0:
        half = height // 2
        far = (me + n_row // 2) % n_row
        along = place(along, lax.ppermute(from_below[:half], "row", up), far, 0)
        along = place(along, lax.ppermute(from_above[half:], "row", down), far, half)

    lower, inverse = cholesky_and_inverse(whole_diag)
    own_rows = diag_block.shape[0]
    factor_diag = lax.dynamic_slice_in_dim(
        lower, lax.axis_index(("row", "col")) * own_rows, own_rows, 0
    )
    row_full = solve(across, inverse)
    col_rows = solve(along, inverse)
    factor_panel = lax.dynamic_slice(
        row_full,
        (lax.axis_index("col") * height, lax.axis_index("depth") * width),
        (height, width),
    )
    schur = trailing - dot_t(col_rows, row_full, lax.Precision.HIGH)
    return (factor_diag, factor_panel, schur)


def solution(mesh):
    in_specs = (P(("row", "col"), None), P(("row", "col"), "depth"), P(("col", "depth"), "row"))
    out_specs = (P(("row", "col"), None), P(("row", "col"), "depth"), P(("col", "depth"), "row"))
    return jax.shard_map(local, mesh=mesh, in_specs=in_specs, out_specs=out_specs, check_vma=False)
```
